128 devices in a mesh: dp: 16 (over z, y), ep: 8 (over x, core).
Axes of the slice: x: 4, y: 4, z: 4, core: 2. Of those that a mesh axis runs over, the one named last changes fastest.
Arguments:
- x_in: bfloat16 [32768, 1536], P(('dp', 'ep'))
- dy_in: bfloat16 [32768, 1536], P(('dp', 'ep'))
- top_ids: int32 [32768, 6], P(('dp', 'ep'))
- w_router: bfloat16 [1536, 64], P(('dp', 'ep'))
- w_gate: bfloat16 [64, 1536, 512], P('ep', 'dp')
- w_up: bfloat16 [64, 1536, 512], P('ep', 'dp')
- w_down: bfloat16 [64, 512, 1536], P('ep', 'dp')
- s_gate: bfloat16 [1536, 1024], P(('dp', 'ep'))
- s_up: bfloat16 [1536, 1024], P(('dp', 'ep'))
- s_down: bfloat16 [1024, 1536], P(('dp', 'ep'))
Outputs:
- output 1: bfloat16 [32768, 1536], P(('dp', 'ep'))
- output 2: bfloat16 [32768, 1536], P(('dp', 'ep'))
- output 3: float32 [1536, 64], P(('dp', 'ep'))
- output 4: float32 [64, 1536, 512], P('ep', 'dp')
- output 5: float32 [64, 1536, 512], P('ep', 'dp')
- output 6: float32 [64, 512, 1536], P('ep', 'dp')
- output 7: float32 [1536, 1024], P(('dp', 'ep'))
- output 8: float32 [1536, 1024], P(('dp', 'ep'))
- output 9: float32 [1024, 1536], P(('dp', 'ep'))
All inputs are finite; a program needn't handle non-finite values.
Results may differ from the reference program's by a relative error of at most 0.00499059.
Values are sent between devices in bfloat16 or wider.
A program may use at most 1 GiB of HBM per device.

```python
import math
import jax
import jax.numpy as jnp
from jax import lax

MODEL_DIM = 1536
NUM_EXPERTS = 64
TOP_K = 6
EXPERT_FF = 512
SHARED_FF = 1024
TOK_DEV = 256
NUM_BLOCKS = 128
SLOT_CAP = 2 * TOK_DEV * TOP_K // NUM_EXPERTS
TOKENS = TOK_DEV * NUM_BLOCKS


def draw_routes(route_key):
    choices = TOK_DEV * TOP_K
    rank_expert = jax.random.permutation(jax.random.fold_in(route_key, 1), NUM_EXPERTS)
    rank_ids = jnp.arange(1, NUM_EXPERTS, dtype=jnp.int32)
    weights = 16384 // (rank_ids + NUM_EXPERTS // 2)
    spare_cnt = choices - SLOT_CAP - (NUM_EXPERTS - 1)
    base_cnt = 1 + (spare_cnt * weights) // jnp.sum(weights)
    short_cnt = spare_cnt - jnp.sum(base_cnt - 1)
    tail_cnt = base_cnt + (rank_ids >= NUM_EXPERTS - short_cnt).astype(jnp.int32)
    counts = jnp.concatenate([jnp.full((1,), SLOT_CAP, dtype=jnp.int32), tail_cnt])
    run_ends = jnp.cumsum(counts)
    slot_rank = jnp.searchsorted(run_ends, jnp.arange(choices, dtype=jnp.int32), side='right')
    id_grid = rank_expert[slot_rank].reshape(TOP_K, TOK_DEV).T
    blk_keys = jax.random.split(jax.random.fold_in(route_key, 2), NUM_BLOCKS)
    blocks = jax.vmap(lambda blk_key: id_grid[jax.random.permutation(blk_key, TOK_DEV)])(blk_keys)
    return blocks.reshape(TOKENS, TOP_K).astype(jnp.int32)


def setup_inputs(seed: int = 0) -> dict:
    sub_keys = jax.random.split(jax.random.key(seed), 11)
    top_ids = draw_routes(sub_keys[0])
    w_router = (jax.random.normal(sub_keys[1], (MODEL_DIM, NUM_EXPERTS), jnp.float32) * MODEL_DIM ** -0.5).astype(jnp.bfloat16)
    strength = jax.random.uniform(sub_keys[2], (TOKENS, TOP_K), jnp.float32, 0.6, 1.1) * math.log(NUM_EXPERTS)
    picked = (top_ids[:, :, None] == jnp.arange(NUM_EXPERTS)[None, None, :]).astype(jnp.float32)
    coeffs = jnp.einsum('tk,tke->te', strength, picked)
    noise_val = jax.random.normal(sub_keys[3], (TOKENS, MODEL_DIM), jnp.float32)
    x_in = (noise_val + jnp.dot(coeffs, w_router.astype(jnp.float32).T)).astype(jnp.bfloat16)
    dy_in = jax.random.normal(sub_keys[4], (TOKENS, MODEL_DIM), jnp.float32).astype(jnp.bfloat16)
    w_gate = (jax.random.normal(sub_keys[5], (NUM_EXPERTS, MODEL_DIM, EXPERT_FF), jnp.float32) * MODEL_DIM ** -0.5).astype(jnp.bfloat16)
    w_up = (jax.random.normal(sub_keys[6], (NUM_EXPERTS, MODEL_DIM, EXPERT_FF), jnp.float32) * MODEL_DIM ** -0.5).astype(jnp.bfloat16)
    w_down = (jax.random.normal(sub_keys[7], (NUM_EXPERTS, EXPERT_FF, MODEL_DIM), jnp.float32) * EXPERT_FF ** -0.5).astype(jnp.bfloat16)
    s_gate = (jax.random.normal(sub_keys[8], (MODEL_DIM, SHARED_FF), jnp.float32) * MODEL_DIM ** -0.5).astype(jnp.bfloat16)
    s_up = (jax.random.normal(sub_keys[9], (MODEL_DIM, SHARED_FF), jnp.float32) * MODEL_DIM ** -0.5).astype(jnp.bfloat16)
    s_down = (jax.random.normal(sub_keys[10], (SHARED_FF, MODEL_DIM), jnp.float32) * (0.5 * SHARED_FF ** -0.5)).astype(jnp.bfloat16)
    return {'x_in': x_in, 'dy_in': dy_in, 'top_ids': top_ids, 'w_router': w_router, 'w_gate': w_gate, 'w_up': w_up, 'w_down': w_down, 's_gate': s_gate, 's_up': s_up, 's_down': s_down}


def slot_tables(top_blk):
    flat_ids = top_blk.reshape(-1)
    sort_order = jnp.argsort(flat_ids, stable=True)
    counts = jnp.bincount(flat_ids, length=NUM_EXPERTS)
    starts = jnp.cumsum(counts) - counts
    slot_idx = jnp.arange(SLOT_CAP)
    is_valid = slot_idx[None, :] < counts[:, None]
    assign = sort_order[jnp.minimum(starts[:, None] + slot_idx[None, :], TOK_DEV * TOP_K - 1)]
    inverse = jnp.argsort(sort_order, stable=True)
    slot_pos = flat_ids * SLOT_CAP + inverse - starts[flat_ids]
    return assign, is_valid, slot_pos


def silu_grads(d_hidden, gate_pre, up_pre):
    sig_gate = jax.nn.sigmoid(gate_pre)
    silu_gate = gate_pre * sig_gate
    d_gate = (d_hidden * up_pre * sig_gate * (1.0 + gate_pre * (1.0 - sig_gate))).astype(jnp.bfloat16)
    d_up = (d_hidden * silu_gate).astype(jnp.bfloat16)
    return d_gate, d_up


def reference(x_in, dy_in, top_ids, w_router, w_gate, w_up, w_down, s_gate, s_up, s_down):
    logits = jnp.dot(x_in, w_router, preferred_element_type=jnp.float32)
    router_prob = jax.nn.softmax(logits, axis=-1)
    picked = (top_ids[:, :, None] == jnp.arange(NUM_EXPERTS)[None, None, :]).astype(jnp.float32)
    gate_vals = jnp.einsum('tke,te->tk', picked, router_prob)
    gate_f32 = w_gate.astype(jnp.float32)
    up_f32 = w_up.astype(jnp.float32)
    down_f32 = w_down.astype(jnp.float32)

    def block_step(acc_grads, blk_data):
        x_blk, dy_blk, top_blk, gate_blk = blk_data
        assign, is_valid, slot_pos = slot_tables(top_blk)
        src_tok = assign // TOP_K
        rows_x = jnp.where(is_valid[:, :, None], x_blk[src_tok], 0).astype(jnp.float32)
        slot_gate = jnp.where(is_valid, gate_blk.reshape(-1)[assign], 0.0)
        rows_g = (slot_gate[:, :, None] * dy_blk[src_tok].astype(jnp.float32)).astype(jnp.bfloat16).astype(jnp.float32)
        gate_pre = jnp.einsum('ecd,edf->ecf', rows_x, gate_f32)
        up_pre = jnp.einsum('ecd,edf->ecf', rows_x, up_f32)
        hidden = (jax.nn.silu(gate_pre) * up_pre).astype(jnp.bfloat16).astype(jnp.float32)
        out_rows = jnp.einsum('ecf,efd->ecd', hidden, down_f32).astype(jnp.bfloat16)
        d_hidden = jnp.einsum('ecd,efd->ecf', rows_g, down_f32)
        d_gate, d_up = silu_grads(d_hidden, gate_pre, up_pre)
        d_gate = d_gate.astype(jnp.float32)
        d_up = d_up.astype(jnp.float32)
        gw_gate = acc_grads[0] + jnp.einsum('ecd,ecf->edf', rows_x, d_gate)
        gw_up = acc_grads[1] + jnp.einsum('ecd,ecf->edf', rows_x, d_up)
        gw_down = acc_grads[2] + jnp.einsum('ecf,ecd->efd', hidden, rows_g)
        dx_rows = (jnp.einsum('ecf,edf->ecd', d_gate, gate_f32) + jnp.einsum('ecf,edf->ecd', d_up, up_f32)).astype(jnp.bfloat16)
        out_tok = out_rows.reshape(-1, MODEL_DIM)[slot_pos].reshape(TOK_DEV, TOP_K, MODEL_DIM).astype(jnp.float32)
        dx_tok = dx_rows.reshape(-1, MODEL_DIM)[slot_pos].reshape(TOK_DEV, TOP_K, MODEL_DIM).astype(jnp.float32)
        routed = jnp.sum(gate_blk[:, :, None] * out_tok, axis=1)
        gate_grad = jnp.einsum('td,tkd->tk', dy_blk.astype(jnp.float32), out_tok)
        dx_routed = jnp.sum(dx_tok, axis=1)
        return (gw_gate, gw_up, gw_down), (routed, gate_grad, dx_routed)

    zero_gate = jnp.zeros((NUM_EXPERTS, MODEL_DIM, EXPERT_FF), jnp.float32)
    zero_down = jnp.zeros((NUM_EXPERTS, EXPERT_FF, MODEL_DIM), jnp.float32)
    blk_inputs = (x_in.reshape(NUM_BLOCKS, TOK_DEV, MODEL_DIM), dy_in.reshape(NUM_BLOCKS, TOK_DEV, MODEL_DIM), top_ids.reshape(NUM_BLOCKS, TOK_DEV, TOP_K), gate_vals.reshape(NUM_BLOCKS, TOK_DEV, TOP_K))
    grads_out, per_blk = lax.scan(block_step, (zero_gate, zero_gate, zero_down), blk_inputs)
    routed = per_blk[0].reshape(TOKENS, MODEL_DIM)
    gate_grad = per_blk[1].reshape(TOKENS, TOP_K)
    dx_routed = per_blk[2].reshape(TOKENS, MODEL_DIM)

    sg_pre = jnp.dot(x_in, s_gate, preferred_element_type=jnp.float32)
    su_pre = jnp.dot(x_in, s_up, preferred_element_type=jnp.float32)
    s_hidden = (jax.nn.silu(sg_pre) * su_pre).astype(jnp.bfloat16)
    s_out = jnp.dot(s_hidden, s_down, preferred_element_type=jnp.float32)
    y_out = (routed + s_out).astype(jnp.bfloat16)

    d_prob = jnp.einsum('tke,tk->te', picked, gate_grad)
    d_logit = (router_prob * (d_prob - jnp.sum(router_prob * d_prob, axis=-1, keepdims=True))).astype(jnp.bfloat16)
    dw_router = jnp.dot(x_in.T, d_logit, preferred_element_type=jnp.float32)
    dx_router = jnp.dot(d_logit, w_router.T, preferred_element_type=jnp.float32)
    ds_hidden = jnp.dot(dy_in, s_down.T, preferred_element_type=jnp.float32)
    ds_gate_pre, ds_up_pre = silu_grads(ds_hidden, sg_pre, su_pre)
    ds_down = jnp.dot(s_hidden.T, dy_in, preferred_element_type=jnp.float32)
    ds_gate = jnp.dot(x_in.T, ds_gate_pre, preferred_element_type=jnp.float32)
    ds_up = jnp.dot(x_in.T, ds_up_pre, preferred_element_type=jnp.float32)
    dx_shared = jnp.dot(ds_gate_pre, s_gate.T, preferred_element_type=jnp.float32) + jnp.dot(ds_up_pre, s_up.T, preferred_element_type=jnp.float32)
    dx_out = (dx_routed + dx_shared + dx_router).astype(jnp.bfloat16)
    return (y_out, dx_out, dw_router, grads_out[0], grads_out[1], grads_out[2], ds_gate, ds_up, ds_down)
```

```python
import jax
import jax.numpy as jnp
from jax import lax
from jax.sharding import Mesh, PartitionSpec as P

Z, Y, X, C = 4, 4, 4, 2
ALL = ('z', 'y', 'x', 'c')
PLANE = ('y', 'x', 'c')


def silu_grads(d_hidden, gate_pre, up_pre):
    sig_gate = jax.nn.sigmoid(gate_pre)
    silu_gate = gate_pre * sig_gate
    d_gate = (d_hidden * up_pre * sig_gate * (1.0 + gate_pre * (1.0 - sig_gate))).astype(jnp.bfloat16)
    d_up = (d_hidden * silu_gate).astype(jnp.bfloat16)
    return d_gate, d_up


def mm(spec, a, b):
    return jnp.einsum(spec, a, b, preferred_element_type=jnp.float32)


def split3(v):
    hi = lax.reduce_precision(v, 8, 7)
    mid = lax.reduce_precision(v - hi, 8, 7)
    return hi, mid, v - hi - mid


def solution(mesh):
    fine = Mesh(mesh.devices.reshape(Z, Y, X, C), ALL)
    row_spec = P(ALL, None)
    expert_spec = P(('x', 'c'), ('z', 'y'), None)
    bf16 = jnp.bfloat16

    def local_step(x_loc, dy_loc, top_loc, wr_loc, wg_loc, wu_loc, wd_loc, sg_loc, su_loc, sd_loc):
        tok, top_k = top_loc.shape
        dim = x_loc.shape[1]
        experts = wr_loc.shape[1]
        cap = 2 * tok * top_k // experts
        planes = Y * X * C
        per_dev = experts // planes
        half = planes * cap

        def order_cols(w):
            return w.reshape(w.shape[0], X * C, Y, per_dev).transpose(0, 3, 2, 1).reshape(w.shape[0], experts)

        def unorder_cols(w):
            return w.reshape(w.shape[0], per_dev, Y, X * C).transpose(0, 3, 2, 1).reshape(w.shape[0], experts)

        sff = sg_loc.shape[1]
        pad = jnp.zeros((wr_loc.shape[0], 128 - experts), bf16)
        pack = jnp.concatenate([sg_loc, su_loc, sd_loc.reshape(-1, sff), order_cols(wr_loc), pad], axis=1)
        pack = lax.all_gather(pack[None], ALL, axis=0, tiled=True)
        s_down = pack[:, :, 2 * sff:3 * sff].reshape(sff, dim)
        s_both = pack[:, :, :2 * sff].reshape(dim, 2 * sff)
        s_gate, s_up = s_both[:, :sff], s_both[:, sff:]
        w_router = pack[:, :, 3 * sff:3 * sff + experts].reshape(dim, experts)

        ff = wg_loc.shape[2]
        cols = dim // ff
        wd_cut = jnp.concatenate([wd_loc[:, :, q * ff:(q + 1) * ff] for q in range(cols)], axis=1)
        w_all = jnp.concatenate([wg_loc, wu_loc, wd_cut], axis=2)
        w_all = lax.all_to_all(w_all, 'y', 0, 1, tiled=True)
        w_all = lax.all_gather(w_all, 'z', axis=1, tiled=True)
        w_gate, w_up, w_down = w_all[:, :, :ff], w_all[:, :, ff:2 * ff], w_all[:, :, 2 * ff:]
        w_down = w_down.reshape(per_dev, Z * Y, cols, -1, ff).transpose(0, 1, 3, 2, 4).reshape(per_dev, ff, dim)

        ids = (top_loc % per_dev) * planes + ((top_loc // per_dev) % Y) * (X * C) + top_loc // (per_dev * Y)
        chosen = jnp.any(ids.T[:, None, :] == jnp.arange(experts)[None, :, None], axis=0)
        before = jnp.arange(tok)[:, None] < jnp.arange(tok)[None, :]
        rank = mm('es,st->et', chosen.astype(bf16), before.astype(bf16))
        slot = jnp.where(chosen, rank, -1.0)
        hit = slot[:, None, :] == jnp.arange(cap, dtype=jnp.float32)[None, :, None]
        disp = hit.astype(bf16).reshape(per_dev, half, tok)

        def exchange(rows):
            rows = lax.all_to_all(rows.reshape(planes, cap, dim), PLANE, 0, 0, tiled=True)
            return rows.reshape(half, dim)

        recv_x = [exchange(mm('st,td->sd', disp[l], x_loc).astype(bf16)) for l in range(per_dev)]

        prob = jax.nn.softmax(mm('td,de->et', x_loc, w_router), axis=0)
        slot_gate = jnp.sum(jnp.where(hit, prob[:, None, :], 0.0), axis=2).reshape(per_dev, half)
        recv_g = [exchange((slot_gate[l][:, None] * mm('st,td->sd', disp[l], dy_loc)).astype(bf16))
                  for l in range(per_dev)]

        sg_pre = mm('td,df->tf', x_loc, s_gate)
        su_pre = mm('td,df->tf', x_loc, s_up)
        s_hidden = (jax.nn.silu(sg_pre) * su_pre).astype(bf16)
        s_out = mm('tf,fd->td', s_hidden, s_down)
        ds_hidden = mm('td,fd->tf', dy_loc, s_down)
        ds_gate_pre, ds_up_pre = silu_grads(ds_hidden, sg_pre, su_pre)
        gs_down = mm('tf,td->fd', s_hidden, dy_loc)
        ds_both = jnp.concatenate([ds_gate_pre, ds_up_pre], axis=1)
        gs_both = mm('td,tf->df', x_loc, ds_both)
        dx_shared = mm('tf,df->td', ds_both, s_both)

        def scatter_shared(g):
            g = lax.psum_scatter(g, ('z', 'y'), scatter_dimension=0, tiled=True)
            g = g.reshape(X * C, -1, g.shape[1])
            return jnp.sum(lax.all_to_all(g, ('x', 'c'), 0, 0, tiled=True), axis=0)

        o_gs_both, o_gs_down = scatter_shared(gs_both), scatter_shared(gs_down)

        back_o, pre = [], []
        for l in range(per_dev):
            gate_pre = mm('sd,df->sf', recv_x[l], w_gate[l])
            up_pre = mm('sd,df->sf', recv_x[l], w_up[l])
            hidden = (jax.nn.silu(gate_pre) * up_pre).astype(bf16)
            back_o.append(exchange(mm('sf,fd->sd', hidden, w_down[l]).astype(bf16)))
            pre.append((gate_pre, up_pre, hidden))
        back_dx, gw_gate, gw_up, gw_down = [], [], [], []
        for l in range(per_dev):
            gate_pre, up_pre, hidden = pre[l]
            d_hidden = mm('sd,fd->sf', recv_g[l], w_down[l])
            d_gate, d_up = silu_grads(d_hidden, gate_pre, up_pre)
            back_dx.append(exchange((mm('sf,df->sd', d_gate, w_gate[l]) + mm('sf,df->sd', d_up, w_up[l])).astype(bf16)))
            gw_down.append(mm('sf,sd->fd', hidden, recv_g[l]))
            gw_gate.append(mm('sd,sf->df', recv_x[l], d_gate))
            gw_up.append(mm('sd,sf->df', recv_x[l], d_up))

        def scatter_expert(g):
            g = lax.psum_scatter(jnp.stack(g), 'z', scatter_dimension=1, tiled=True)
            return lax.all_to_all(g, 'y', 1, 0, tiled=True)

        o_gw_down, o_gw_gate, o_gw_up = scatter_expert(gw_down), scatter_expert(gw_gate), scatter_expert(gw_up)

        parts = [jnp.where(hit, v[:, None, :], 0.0).astype(bf16).reshape(per_dev, half, tok) for v in split3(prob)]
        routed = sum(mm('st,sd->td', part[l], back_o[l]) for l in range(per_dev) for part in parts)
        y_loc = (routed + s_out).astype(bf16)

        score = jnp.stack([mm('sd,td->st', back_o[l], dy_loc) for l in range(per_dev)])
        d_prob = jnp.sum(jnp.where(hit, score.reshape(experts, cap, tok), 0.0), axis=1)
        d_logit = (prob * (d_prob - jnp.sum(prob * d_prob, axis=0, keepdims=True))).astype(bf16)
        gw_router = mm('td,et->de', x_loc, d_logit).reshape(Z * planes, -1, experts)
        o_gw_router = jnp.sum(lax.all_to_all(gw_router, ALL, 0, 0, tiled=True), axis=0)
        dx_router = mm('et,de->td', d_logit, w_router)

        dx_routed = sum(mm('st,sd->td', disp[l], back_dx[l]) for l in range(per_dev))
        dx_loc = (dx_routed + dx_shared + dx_router).astype(bf16)
        return (y_loc, dx_loc, unorder_cols(o_gw_router), o_gw_gate, o_gw_up, o_gw_down,
                o_gs_both[:, :sff], o_gs_both[:, sff:], o_gs_down)

    return jax.shard_map(local_step, mesh=fine,
                         in_specs=(row_spec, row_spec, row_spec, row_spec, expert_spec, expert_spec, expert_spec, row_spec, row_spec, row_spec),
                         out_specs=(row_spec, row_spec, row_spec, expert_spec, expert_spec, expert_spec, row_spec, row_spec, row_spec),
                         check_vma=False)
```
